512 devices in a mesh: groups: 2 (over y), tok: 32 (over z), head: 8 (over x, core).
Axes of the slice: x: 4, y: 2, z: 32, core: 2. Of those that a mesh axis runs over, the one named last changes fastest.
The devices are a block of a 4x8x32 slice.
Arguments:
- hidden: bfloat16 [20480, 8192], P(('groups', 'tok'), 'head'), parts along dimension 0, may hold values from -6 to 6
- positions: int32 [20480], P(('groups', 'tok')), parts along dimension 0, may hold values from 0 to 10239, as said below
- norm_gain: float32 [8192], P('head'), may hold values from 0.1 to 1.9
- w_key: bfloat16 [8192, 1024], P('head'), may hold values from -0.0625 to 0.0625
- w_value: bfloat16 [8192, 1024], P('head'), may hold values from -0.0625 to 0.0625
- queries: bfloat16 [512, 8192], P(('groups', 'tok'), 'head'), parts along dimension 0, may hold values from -400 to 400
- lengths: int32 [512], P(('groups', 'tok')), parts along dimension 0, may hold values from 1 to 10240
Outputs:
- attended: bfloat16 [512, 8192], P(('groups', 'tok'), 'head'), parts along dimension 0
The draws below stay inside these ranges and needn't reach their ends.
There are 2 independent parts, one for each index of `groups`. The reference program is written for one: setup_inputs(seed, part) draws one part's arguments, and reference() takes and returns one part's arrays. A program takes and returns all parts, laid end to end along the dimension named above; an argument that names none is the same for every part. Nothing has to cross between parts.
Inputs may be any that keep to these rules, and one draw needn't show every extreme that they name: `positions`: each of 0 to 10239 appears once.
All inputs are finite; a program needn't handle non-finite values.
Results may differ from the reference program's by a relative error of at most 0.025.
The reference program's roundings to bfloat16 on the way (of `normed`, `keys`, `values` and `weights`) count: a program that leaves them out, or rounds other values in their place, can miss the bound.
Values may be sent and summed in bfloat16 or wider, within the bound.
No kernel may reach another device: no remote copies, remote signals or barrier semaphores. Data moves between devices by JAX's collectives and lax.ppermute only.
A program may use at most 64 MiB of HBM per device.

```python
import jax
import jax.numpy as jnp
from jax import lax

D = 8192
KVH = 8
HD = 128
QPK = 8
ROWS = 256
QH = 64
PREFIX = 10240


def draw_positions(key, part):
    pages = PREFIX // 8
    order = jax.random.permutation(jax.random.fold_in(key, 11), pages).astype(jnp.int32)
    index = jnp.arange(PREFIX, dtype=jnp.int32)
    return order[index // 8] * 8 + index % 8


def draw_queries(key, part):
    base = jax.random.truncated_normal(jax.random.fold_in(key, 23), -6.0, 6.0, (ROWS, QH * HD), jnp.float32)
    return base.astype(jnp.bfloat16)


def plant(drawn, rng, least, top_value):
    dims = drawn.shape
    index_at = [jax.random.randint(jax.random.fold_in(rng, axis), (), 0, dims[axis]) for axis in range(len(dims))]
    drawn = drawn.at[tuple(index_at)].set(least)
    longest = dims.index(max(dims))
    index_at[longest] = (index_at[longest] + 1) % dims[longest]
    return drawn.at[tuple(index_at)].set(top_value)


def shard_levels(key, dims, shards, low, high):
    factor_of, own = 1.0, jax.random.fold_in(key, 6)
    for position, shards_of in shards:
        heights = jnp.exp(jax.random.uniform(jax.random.fold_in(own, position), (shards_of,), jnp.float32, low / len(shards), high / len(shards)))
        factor_of = factor_of * jnp.repeat(heights, dims[position] // shards_of).reshape([-1 if axis == position else 1 for axis in range(len(dims))])
    return factor_of


def normal_values(rng, dims, spread, most, pieces=(), kind=jnp.bfloat16):
    level = shard_levels(rng, dims, pieces, -0.22, 0.18) if pieces else 1.0
    drawn = jax.random.normal(rng, dims, jnp.float32) * spread * level
    return jnp.minimum(jnp.maximum(drawn, -most), most).astype(kind)


def setup_inputs(seed: int = 0, part: int = 0) -> dict:
    splits = jax.random.split(jax.random.key(seed), 8)
    own_keys = jax.random.split(jax.random.fold_in(splits[7], part), 8)
    return {
        "hidden": normal_values(own_keys[0], (PREFIX, D), 1.0, 6.0, ((0, 32), (1, 8))),
        "positions": draw_positions(jax.random.fold_in(jax.random.fold_in(splits[7], part), 71), part),
        "norm_gain": jnp.clip(1.0 + 0.18 * jax.random.normal(splits[2], (D,), jnp.float32), 0.1, 1.9),
        "w_key": normal_values(splits[3], (D, KVH * HD), D ** -0.5, 0.0625, ((0, 8),)),
        "w_value": normal_values(splits[4], (D, KVH * HD), D ** -0.5, 0.0625, ((0, 8),)),
        "queries": draw_queries(jax.random.fold_in(jax.random.fold_in(splits[7], part), 71), part),
        "lengths": plant(jax.random.randint(own_keys[6], (ROWS,), 1, PREFIX + 1), jax.random.fold_in(own_keys[6], 1), 1, PREFIX).astype(jnp.int32),
    }


def rotate_keys(keys, positions):
    half = HD // 2
    freq = 500000.0 ** (-(jnp.arange(half, dtype=jnp.float32) * 2.0) / HD)
    angle = positions.astype(jnp.float32)[:, None] * freq[None, :]
    cosine = jnp.cos(angle)[:, None, :]
    sine = jnp.sin(angle)[:, None, :]
    first = keys[..., :half]
    second = keys[..., half:]
    return jnp.concatenate([first * cosine - second * sine, second * cosine + first * sine], axis=-1)

def reference(hidden, positions, norm_gain, w_key, w_value, queries, lengths):
    wide = hidden.astype(jnp.float32)
    meansq = lax.optimization_barrier(jnp.mean(wide * wide, axis=1, keepdims=True))
    normed = (wide * lax.rsqrt(meansq + 1e-05) * norm_gain).astype(jnp.bfloat16)
    key_raw = jnp.dot(normed, w_key, preferred_element_type=jnp.float32).reshape(PREFIX, KVH, HD)
    keys = rotate_keys(key_raw, positions).astype(jnp.bfloat16)
    values = jnp.dot(normed, w_value, preferred_element_type=jnp.float32).astype(jnp.bfloat16).reshape(PREFIX, KVH, HD)
    valid = positions[None, :] < lengths[:, None]
    grouped = queries.reshape(ROWS, KVH, QPK, HD)
    scale = HD ** (-0.5)

    def one_head(index):
        query_head = grouped[:, index]
        key_head = keys[:, index]
        value_head = values[:, index]
        scores = jnp.einsum('rgd,pd->rgp', query_head.astype(jnp.float32), key_head.astype(jnp.float32)) * scale
        scores = jnp.where(valid[:, None, :], scores, -1e+30)
        top = lax.optimization_barrier(jnp.max(scores, axis=2, keepdims=True))
        weights = jnp.exp(scores - top).astype(jnp.bfloat16)
        numer = jnp.einsum('rgp,pd->rgd', weights.astype(jnp.float32), value_head.astype(jnp.float32))
        denom = lax.optimization_barrier(jnp.sum(weights.astype(jnp.float32), axis=2, keepdims=True))
        return numer / denom
    result = lax.map(one_head, jnp.arange(KVH, dtype=jnp.int32))
    return result.transpose(1, 0, 2, 3).reshape(ROWS, QH * HD).astype(jnp.bfloat16)
```

```python
import functools

import jax
import jax.numpy as jnp
from jax import lax
from jax.experimental import pallas as pl
from jax.experimental.pallas import tpu as pltpu
from jax.sharding import PartitionSpec as P

HD = 128
QPK = 8
NEAR = 4
CODE = 128

F32 = jnp.float32
BF16 = jnp.bfloat16


def call(kernel, out, *args, **kw):
    return pl.pallas_call(kernel, out_shape=jax.ShapeDtypeStruct(*out), **kw)(*args)


def diagonal(n):
    return lax.broadcasted_iota(jnp.int32, (n, n), 0) == lax.broadcasted_iota(jnp.int32, (n, n), 1)


def squares_kernel(hidden, out):
    tokens = hidden.shape[0]
    wide = hidden[...].astype(F32)
    column = jnp.sum(wide * wide, axis=1, keepdims=True)
    eye = diagonal(128)
    rows = []
    for at in range(0, 1024, 128):
        if at < tokens:
            part = column[at : min(at + 128, tokens)]
            if part.shape[0] < 128:
                part = jnp.concatenate([part, jnp.zeros((128 - part.shape[0], 1), F32)], axis=0)
            rows.append(jnp.sum(jnp.where(eye, part, 0.0), axis=0, keepdims=True))
        else:
            rows.append(jnp.zeros((1, 128), F32))
    tile = jnp.concatenate(rows, axis=0)
    for peer in range(out.shape[0]):
        out[peer] = tile


def project_kernel(full_width, sums, hidden, gain, w_key, w_value, out, normed):
    tokens = hidden.shape[0]

    @pl.when(pl.program_id(0) == 0)
    def _():
        total = sums[0]
        for peer in range(1, sums.shape[0]):
            total = total + sums[peer]
        rate = lax.rsqrt(total / full_width + 1e-05)
        eye = diagonal(128)
        columns = []
        for at in range(0, tokens, 128):
            row = rate[at // 128 : at // 128 + 1]
            columns.append(jnp.sum(jnp.where(eye, row, 0.0), axis=1, keepdims=True))
        column = jnp.concatenate(columns, axis=0)[:tokens]
        normed[...] = (hidden[...].astype(F32) * column * gain[...]).astype(BF16)

    x = normed[...]
    k = jnp.dot(x, w_key[...], preferred_element_type=F32)
    v = jnp.dot(x, w_value[...], preferred_element_type=F32)
    for core in range(2):
        out[core, 0, :, :HD] = k[:, core * HD : (core + 1) * HD]
        out[core, 0, :, HD:] = v[:, core * HD : (core + 1) * HD]


def pack_kernel(parts, out):
    for x in range(out.shape[0]):
        k = parts[0, x, :, :HD] + parts[1, x, :, :HD]
        v = parts[0, x, :, HD:] + parts[1, x, :, HD:]
        high = k.astype(BF16)
        out[x, :, :HD] = high
        out[x, :, HD : 2 * HD] = (k - high.astype(F32)).astype(BF16)
        out[x, :, 2 * HD :] = v.astype(BF16)


def rotate_kernel(parts, cosine, sine, coded, out):
    tokens = parts.shape[1]
    k = jnp.zeros((tokens, HD), F32)
    v = jnp.zeros((tokens, HD), F32)
    for x in range(parts.shape[0]):
        k = k + (parts[x, :, :HD].astype(F32) + parts[x, :, HD : 2 * HD].astype(F32))
        v = v + parts[x, :, 2 * HD :].astype(F32)
    k = k * cosine[...] + pltpu.roll(k, HD // 2, 1) * sine[...]
    keys, values, where = k.astype(BF16), v.astype(BF16), coded[...]
    for peer in range(out.shape[0]):
        out[peer, :tokens, :HD] = keys
        out[peer, :tokens, HD:] = values
        out[peer, tokens:, :] = where


def attend_kernel(tokens, queries, kv, out):
    far, own = queries.shape[0], queries.shape[1]
    rows = far * own
    wide = QPK * HD
    q = []
    for h in range(QPK):
        q.append(queries[:, :, h * HD : (h + 1) * HD].astype(F32).reshape(rows, HD).astype(BF16))
    q = jnp.concatenate(q, axis=0)
    code = queries[:, :, wide:].astype(F32).reshape(rows, -1)
    length = code[:, 0:1] * CODE + code[:, 1:2]
    length = jnp.concatenate([length] * QPK, axis=0)
    scores, top = [], None
    for s in range(kv.shape[0]):
        k = kv[s, :tokens, :HD]
        x = lax.dot_general(q, k, (((1,), (1,)), ((), ())), preferred_element_type=F32) * HD**-0.5
        spare = kv[s, tokens:, :].astype(F32)
        width = spare.shape[1]
        pieces = []
        for i in range(0, tokens, width):
            take = min(width, tokens - i)
            n = i // width
            pieces.append(spare[n : n + 1, :take] * CODE + spare[8 + n : 9 + n, :take])
        place = jnp.concatenate(pieces, axis=1)
        x = jnp.where(place < length, x, -1e30)
        scores.append(x)
        here = jnp.max(x, axis=1, keepdims=True)
        top = here if top is None else jnp.maximum(top, here)
    numer = jnp.zeros((QPK * rows, HD), F32)
    denom = jnp.zeros((QPK * rows, 1), F32)
    for s in range(kv.shape[0]):
        w = jnp.exp(scores[s] - top).astype(BF16)
        denom = denom + jnp.sum(w.astype(F32), axis=1, keepdims=True)
        numer = numer + jnp.dot(w, kv[s, :tokens, HD:], preferred_element_type=F32)
    lane = lax.broadcasted_iota(jnp.int32, (rows, HD), 1)
    meta = jnp.zeros((rows, HD), F32)
    for h in range(QPK):
        part = slice(h * rows, (h + 1) * rows)
        out[:, :, h * HD : (h + 1) * HD] = numer[part].reshape(far, own, HD).astype(BF16)
        values = []
        for x, count in ((top[part], 3), (denom[part], 2)):
            for _ in range(count):
                high = x.astype(BF16).astype(F32)
                values.append(high)
                x = x - high
        for i, x in enumerate(values):
            meta = jnp.where(lane == 5 * h + i, x, meta)
    out[:, :, wide:] = meta.reshape(far, own, HD).astype(BF16)


def merge_kernel(parts, out):
    wide = QPK * HD
    meta = parts[:, :, wide:].astype(F32)
    for h in range(QPK):
        at = 5 * h
        top = meta[:, :, at : at + 1] + meta[:, :, at + 1 : at + 2] + meta[:, :, at + 2 : at + 3]
        denom = meta[:, :, at + 3 : at + 4] + meta[:, :, at + 4 : at + 5]
        scale = jnp.exp(top - jnp.max(top, axis=0, keepdims=True))
        numer = jnp.sum(parts[:, :, h * HD : (h + 1) * HD].astype(F32) * scale, axis=0)
        out[:, h * HD : (h + 1) * HD] = (numer / jnp.sum(denom * scale, axis=0)).astype(BF16)


def coded_pair(x):
    return (x // CODE).astype(BF16), (x % CODE).astype(BF16)


def body(hidden, positions, norm_gain, w_key, w_value, queries, lengths):
    tokens, width = hidden.shape
    heads, toks = lax.axis_size("head"), lax.axis_size("tok")
    chips = heads // 2
    far = toks // NEAR
    own = queries.shape[0]
    cores = [[2 * x, 2 * x + 1] for x in range(chips)]
    row = [[2 * x + c for x in range(chips)] for c in range(2)]
    near = [[NEAR * b + i for i in range(NEAR)] for b in range(far)]
    stride = [[NEAR * b + i for b in range(far)] for i in range(NEAR)]

    high, low = coded_pair(lengths)
    extra = jnp.pad(jnp.stack([high, low], axis=1), ((0, 0), (0, HD - 2)))
    asked = jnp.concatenate([queries, extra], axis=1)
    asked = jnp.broadcast_to(asked[None], (far, *asked.shape))
    asked = lax.all_to_all(asked, "tok", 0, 0, axis_index_groups=stride, tiled=True)

    sums = call(squares_kernel, ((heads, 8, 128), F32), hidden)
    sums = lax.all_to_all(sums, "head", 0, 0, tiled=True)

    half = HD // 2
    freq = 500000.0 ** (-(jnp.arange(half, dtype=F32) * 2.0) / HD)
    angle = positions.astype(F32)[:, None] * freq[None, :]
    cosine, sine = jnp.cos(angle), jnp.sin(angle)
    cosine = jnp.concatenate([cosine, cosine], axis=1)
    sine = jnp.concatenate([-sine, sine], axis=1)
    spare = 8 * 2 * HD - tokens
    coded = jnp.concatenate([jnp.pad(x, (0, spare)).reshape(8, 2 * HD) for x in coded_pair(positions)])

    columns = w_key.shape[1] // chips
    block = lambda *shape: pl.BlockSpec(shape, lambda i: (0,) * len(shape))
    strip = pl.BlockSpec((width, columns), lambda i: (0, i))
    parts = call(
        functools.partial(project_kernel, width * heads),
        ((2, chips, tokens, 2 * HD), F32),
        sums,
        hidden,
        norm_gain[None],
        w_key,
        w_value,
        grid=(chips,),
        in_specs=[block(*sums.shape), block(tokens, width), block(1, width), strip, strip],
        out_specs=pl.BlockSpec((2, 1, tokens, 2 * HD), lambda i: (0, i, 0, 0)),
        scratch_shapes=[pltpu.VMEM((tokens, width), BF16)],
    )
    parts = lax.all_to_all(parts, "head", 0, 0, axis_index_groups=cores, tiled=True)
    parts = call(pack_kernel, ((chips, tokens, 3 * HD), BF16), parts)
    parts = lax.all_to_all(parts, "head", 0, 0, axis_index_groups=row, tiled=True)
    kv = call(rotate_kernel, ((NEAR, tokens + 16, 2 * HD), BF16), parts, cosine, sine, coded)
    kv = lax.all_to_all(kv, "tok", 0, 0, axis_index_groups=near, tiled=True)
    part = call(
        functools.partial(attend_kernel, tokens), ((far, own, QPK * HD + HD), BF16), asked, kv
    )
    part = lax.all_to_all(part, "tok", 0, 0, axis_index_groups=stride, tiled=True)
    return call(merge_kernel, ((own, QPK * HD), BF16), part)


def solution(mesh):
    in_specs = (
        P(("groups", "tok"), "head"),
        P(("groups", "tok")),
        P("head"),
        P("head", None),
        P("head", None),
        P(("groups", "tok"), "head"),
        P(("groups", "tok")),
    )
    out_specs = P(("groups", "tok"), "head")
    return jax.shard_map(body, mesh=mesh, in_specs=in_specs, out_specs=out_specs, check_vma=False)
```
